512 devices in a mesh: rep: 8 (over z_lo, core), blk: 64 (over z_hi, x, y).
Axes of the slice: x: 4, y: 8, z: 8 (z_hi: 2, z_lo: 4; z = z_hi * 4 + z_lo), core: 2. Of those that a mesh axis runs over, the one named last changes fastest.
Arguments:
- gradients: bfloat16 [8, 512, 8, 4096], P('rep', 'blk'), may hold values from -22 to 22
- left_stat: float32 [64, 512, 512], P('blk', 'rep'), as said below
- right_stat: float32 [64, 512, 512], P('blk', 'rep')
- momentum: float32 [64, 512, 512], P('blk', 'rep'), may hold values from -6 to 6
- master: float32 [64, 512, 512], P('blk', 'rep'), may hold values from -6 to 6
Outputs:
- params: bfloat16 [512, 8, 4096], P('blk')
- momentum_out: float32 [64, 512, 512], P('blk', 'rep')
- left_new: float32 [64, 512, 512], P('blk', 'rep')
- right_new: float32 [64, 512, 512], P('blk', 'rep')
The draws below stay inside these ranges and needn't reach their ends.
Inputs may be any that keep to these rules, and one draw needn't show every extreme that they name: Every block of left_stat and right_stat is symmetric positive semidefinite.
All inputs are finite; a program needn't handle non-finite values.
Results may differ from the reference program's by a relative error of at most 0.005.
Values may be sent and summed in bfloat16 or wider, within the bound.
No kernel may reach another device: no remote copies, remote signals or barrier semaphores. Data moves between devices by JAX's collectives and lax.ppermute only.
A program may use at most 64 MiB of HBM per device.

```python
import math
import jax
import jax.numpy as jnp
from jax import lax

B = 512
BCOLS = 8
ITERS = 4
REPLICAS = 8
BLOCKS = 64
BROWS = 8
COLS = 4096
N_REP = 8


def gram_blocks(key):
    key_matrix, key_scale = jax.random.split(key)
    base_draw = jax.random.normal(key_matrix, (BLOCKS, B, B), jnp.float32)
    gram = jnp.einsum('kij,klj->kil', base_draw, base_draw) / B
    row_scales = jnp.exp(jax.random.uniform(key_scale, (BLOCKS, B), jnp.float32, math.log(0.5), math.log(5.0)))
    return gram * row_scales[:, :, None] * row_scales[:, None, :]


def draw_left_stat(key, part):
    return gram_blocks(jax.random.fold_in(key, 11))


def draw_right_stat(key, part):
    return gram_blocks(jax.random.fold_in(key, 23))


def draw_gradients(key, part):
    key_values = jax.random.fold_in(key, 37)
    key_rows = jax.random.fold_in(key, 41)
    key_cols = jax.random.fold_in(key, 43)
    shape_all = (REPLICAS, B, BROWS, COLS)
    position = jnp.arange(COLS, dtype=jnp.float32) % B / (B - 1)
    slice_rows = B // REPLICAS
    slice_index = jnp.arange(B, dtype=jnp.int32) // slice_rows
    slice_weight = jnp.where(slice_index % 2 == 0, 1.0 + slice_index.astype(jnp.float32) / max(REPLICAS - 1, 1), 0.0)
    row_factor = jnp.clip(jax.random.normal(key_rows, (B, BROWS, BCOLS), jnp.float32), -4.0, 4.0) * slice_weight[:, None, None]
    col_factor = jnp.clip(jax.random.normal(key_cols, (BROWS, BCOLS, B), jnp.float32), -4.0, 4.0)
    common = (row_factor[:, :, :, None] * col_factor[None, :, :, :]).reshape(B, BROWS, COLS)
    strength = 2.4 * B ** (-0.25) / math.sqrt(REPLICAS)
    base_draw = jnp.clip(jax.random.normal(key_values, shape_all, jnp.float32), -6.0, 6.0)
    column_scale = jnp.exp(math.log(0.3) + position * math.log(10.0))
    values = 0.6 * (base_draw + strength * common[None]) * column_scale
    return jnp.clip(values, -22.0, 22.0).astype(jnp.bfloat16)


def levels(stream_key, extent, shards, smallest, high):
    def one(dim, blocks):
        steps = jax.random.uniform(jax.random.fold_in(jax.random.fold_in(stream_key, 6), dim), (blocks,), jnp.float32, smallest / len(shards), high / len(shards))
        return jnp.repeat(jnp.exp(steps), extent[dim] // blocks).reshape((-1,) + (1,) * (len(extent) - dim - 1))

    level = one(*shards[0])
    for cut in shards[1:]:
        level = level * one(*cut)
    return level


def noise(own_key, extent, deviation, limit, shards=(), kind=jnp.bfloat16):
    result = deviation * jax.random.normal(own_key, extent, jnp.float32)
    if shards:
        result = result * levels(own_key, extent, shards, -0.22, 0.18)
    return jnp.clip(result, -limit, limit).astype(kind)


def setup_inputs(seed: int = 0) -> dict:
    key_of = jax.random.split(jax.random.key(seed), 6)
    gradients = draw_gradients(jax.random.fold_in(key_of[5], 71), 0)
    left_stat = draw_left_stat(jax.random.fold_in(key_of[5], 71), 0)
    right_stat = draw_right_stat(jax.random.fold_in(key_of[5], 71), 0)
    momentum = noise(key_of[3], (BLOCKS, B, B), 1.0, 6.0, ((0, 64), (1, 8)), jnp.float32)
    master = noise(key_of[4], (BLOCKS, B, B), 1.0, 6.0, ((0, 64), (1, 8)), jnp.float32)
    return dict(gradients=gradients, left_stat=left_stat, right_stat=right_stat, momentum=momentum, master=master)


stat_decay = 0.9
moment_decay = 0.9
step_size = 0.25

def exact_dot(left, right):
    return jnp.dot(left, right, precision=lax.Precision.HIGHEST, preferred_element_type=jnp.float32)

def inverse_root(stat):
    identity = jnp.eye(stat.shape[0], dtype=jnp.float32)
    frob_norm = jnp.sqrt(jnp.sum(stat * stat))
    root_scale = jnp.sqrt(jnp.sqrt(frob_norm))
    iterate = stat / frob_norm
    root = identity
    for sweep_index in range(ITERS):
        factor = (5.0 * identity - iterate) * 0.25
        if sweep_index == 0:
            root = factor / root_scale
        else:
            root = exact_dot(root, factor)
        if sweep_index + 1 < ITERS:
            iterate = exact_dot(exact_dot(exact_dot(exact_dot(factor, factor), factor), factor), iterate)
    return root

def block_update(inputs):
    grad_block, left_old, right_old = inputs
    left_next = stat_decay * left_old + (1.0 - stat_decay) * exact_dot(grad_block, grad_block.T)
    right_next = stat_decay * right_old + (1.0 - stat_decay) * exact_dot(grad_block.T, grad_block)
    precond = exact_dot(exact_dot(inverse_root(left_next), grad_block), inverse_root(right_next))
    return (precond, left_next, right_next)

def reference(gradients, left_stat, right_stat, momentum, master):
    mean_grad = lax.optimization_barrier(jnp.sum(gradients.astype(jnp.float32), axis=0)) * (1.0 / N_REP)
    blocks = mean_grad.reshape(B, BROWS, BCOLS, B).transpose(1, 2, 0, 3).reshape(BLOCKS, B, B)
    precond, left_next, right_next = lax.map(block_update, (blocks, left_stat, right_stat))
    graft_scale = jnp.sqrt(jnp.sum(blocks * blocks)) / jnp.sqrt(jnp.sum(precond * precond))
    moment_new = moment_decay * momentum + graft_scale * precond
    weights = (master - step_size * moment_new).astype(jnp.bfloat16)
    params = weights.reshape(BROWS, BCOLS, B, B).transpose(2, 0, 1, 3).reshape(B, BROWS, COLS)
    return (params, moment_new, left_next, right_next)
```

```python
import functools
import jax
import jax.numpy as jnp
from jax import lax
from jax.experimental import pallas as pl
from jax.experimental.pallas import tpu as pltpu
from jax.sharding import Mesh
from jax.sharding import PartitionSpec as P

REP = ("zl", "co")
COL = ("zh", "x")
BLK = ("zh", "x", "y")
ALL = ("zl", "co", "zh", "x", "y")
FAN = ("zl", "zh", "x")
SIZES = (4, 2, 2, 4, 8)
N = 8
ROWS = 64
BLOCK = 512
ITERS = 4
LANES = 128
WIDE = BLOCK // LANES

stat_decay = 0.9
moment_decay = 0.9
step_size = 0.25

F32 = jnp.float32
BF16 = jnp.bfloat16


def exchanged(pieces, axis):
    return lax.all_to_all(pieces, axis, split_axis=0, concat_axis=0, tiled=True)


def rep_with_y():
    return [
        ((r * N + c) * N + y, (y * N + c) * N + r)
        for r in range(N)
        for c in range(N)
        for y in range(N)
    ]


def three_parts(value):
    high = value.astype(BF16).astype(F32)
    rest = value - high
    middle = rest.astype(BF16).astype(F32)
    return high, middle, rest - middle


def dot(a, b, dims=((1,), (0,))):
    return lax.dot_general(a, b, (dims, ((), ())), preferred_element_type=F32)


def block_kernel(y_ref, g_ref, side_ref, msg_ref, ret_ref, m_f, m_b, v_b, w_f, w_b, g_b, y_f, y_b, z_b):
    own = pl.multiple_of(y_ref[0] * ROWS, ROWS)
    chunk = BLOCK // 2
    spans = [pl.ds(k * chunk, chunk) for k in range(2)]
    norm_g = jnp.zeros((1, 1), F32)
    for rows in spans:
        part = g_ref[rows, :]
        norm_g += jnp.sum(part * part, keepdims=True)
        g_b[rows, :] = part.astype(BF16)
        y_f[rows, :] = part
        y_b[rows, :] = part.astype(BF16)
    scale = jnp.ones((1, 1), F32)
    for side in range(2):
        gram = dot(g_b[...], g_b[...], (((1,), (1,)), ((0,), (0,)))[side])
        w_f[side] = gram
        ret_ref[pl.ds((1 + side) * ROWS, ROWS), :] = w_f[side, pl.ds(own, ROWS), :].astype(BF16)
        total = jnp.zeros((1, 1), F32)
        for k in range(N):
            rows = pl.ds(k * ROWS, ROWS)
            old = side_ref[k, side * ROWS : (side + 1) * ROWS, :].astype(F32)
            new = stat_decay * old + (1.0 - stat_decay) * w_f[side, rows, :]
            m_f[side, rows, :] = new
            total += jnp.sum(new * new, keepdims=True)
        frob = jnp.sqrt(total)
        scale = scale / jnp.sqrt(jnp.sqrt(frob))
        inverse = 1.0 / frob
        for rows in spans:
            new = m_f[side, rows, :] * inverse
            m_f[side, rows, :] = new
            m_b[side, rows, :] = new.astype(BF16)

    def apply_factors():
        for rows in spans:
            new = 1.25 * y_f[rows, :] - 0.25 * dot(m_b[0, rows, :], y_b[...])
            y_f[rows, :] = new
            z_b[rows, :] = new.astype(BF16)
        for rows in spans:
            new = 1.25 * y_f[rows, :] - 0.25 * dot(z_b[rows, :], m_b[1])
            y_f[rows, :] = new
            y_b[rows, :] = new.astype(BF16)

    def sweep(_, carry):
        for side in range(2):
            for rows in spans:
                square = dot(m_b[side, rows, :], m_b[side])
                v_b[side, rows, :] = (0.0625 * square - 0.625 * m_f[side, rows, :]).astype(BF16)
        apply_factors()
        for side in range(2):
            for rows in spans:
                new = 1.5625 * m_f[side, rows, :] + dot(v_b[side, rows, :], m_b[side])
                w_f[side, rows, :] = new
                w_b[side, rows, :] = new.astype(BF16)
        for side in range(2):
            for rows in spans:
                new = 1.5625 * w_f[side, rows, :] + dot(v_b[side, rows, :], w_b[side])
                m_f[side, rows, :] = new
                m_b[side, rows, :] = new.astype(BF16)
        return carry

    lax.fori_loop(0, ITERS - 1, sweep, 0)
    apply_factors()
    norm_p = jnp.zeros((1, 1), F32)
    for rows in spans:
        new = y_f[rows, :] * scale
        norm_p += jnp.sum(new * new, keepdims=True)
        y_f[rows, :] = new
    ret_ref[0:ROWS, :] = y_f[pl.ds(own, ROWS), :].astype(BF16)
    lane = lax.broadcasted_iota(jnp.int32, (16, LANES), 1)
    norms = jnp.zeros((16, LANES), F32)
    for k, part in enumerate(three_parts(norm_p) + three_parts(norm_g)):
        norms = jnp.where(lane == k, part, norms)
    norms = norms.astype(BF16)
    start = y_ref[0] * N
    for c in range(N):
        rows = y_f[pl.ds(pl.multiple_of(c * ROWS + start, N), N), :]
        both = jnp.concatenate([rows, side_ref[c, 2 * ROWS : 2 * ROWS + N, :].astype(F32)], axis=0)
        both = both.astype(BF16)
        for z in range(SIZES[0]):
            msg_ref[z * N + c, :, 0:BLOCK] = both
            msg_ref[z * N + c, :, BLOCK : BLOCK + LANES] = norms


def final_kernel(got_ref, ret_ref, mom_ref, params_ref, mom_out_ref, rows_f):
    total = jnp.zeros((16, LANES), F32)
    for q in range(2):
        for z in range(SIZES[0]):
            for i in range(N):
                total += got_ref[q, z * N + i, :, BLOCK : BLOCK + LANES].astype(F32)
    lane = lax.broadcasted_iota(jnp.int32, (16, LANES), 1)
    norm_p = jnp.sum(jnp.where(lane < 3, total, 0.0), keepdims=True) * (1.0 / 16)
    norm_g = jnp.sum(jnp.where(lane < 3, 0.0, total), keepdims=True) * (1.0 / 16)
    graft = jnp.sqrt(norm_g) / jnp.sqrt(norm_p)
    for z in range(SIZES[0]):
        for q in range(2):
            slot = (z * 2 + q) % 2
            for i in range(N):
                both = got_ref[q, z * N + i, :, 0:BLOCK].astype(F32)
                both = both[N:, :] - step_size * (graft * both[:N, :])
                for w in range(WIDE):
                    rows_f[slot, w, i * N : (i + 1) * N, :] = both[:, w * LANES : (w + 1) * LANES]
            for p in range(N):
                for w in range(WIDE):
                    cols = pl.ds((z * 2 + q) * BLOCK + w * LANES, LANES)
                    params_ref[p, :, cols] = rows_f[slot, w, pl.ds(p, N, stride=N), :].astype(BF16)
    mom_out_ref[...] = moment_decay * mom_ref[...] + graft * ret_ref[0:ROWS, :].astype(F32)


def vmem(count):
    return [pl.BlockSpec(memory_space=pltpu.VMEM)] * count


def on_device(gradients, left_stat, right_stat, momentum, master):
    y = lax.axis_index("y")
    base = (master[0] - (step_size * moment_decay) * momentum[0]).astype(BF16)
    side = jnp.concatenate([left_stat[0].astype(BF16), right_stat[0].astype(BF16), base], axis=0)
    side = lax.ppermute(side, ALL, rep_with_y())
    stats = jnp.broadcast_to(side[None, : 2 * ROWS], (N, 2 * ROWS, BLOCK))
    side = jnp.concatenate([stats, side[2 * ROWS :].reshape(N, N, BLOCK)], axis=1)
    side = exchanged(side, "y")

    pieces = gradients.reshape(N, N, N, BLOCK).transpose(2, 0, 1, 3)
    pieces = exchanged(pieces, REP)
    mean = jnp.sum(pieces.astype(F32), axis=0) * (1.0 / N)
    mean = mean.transpose(1, 0, 2)
    mean = jnp.broadcast_to(mean[:, None], (N, N, N, BLOCK)).reshape(N * N, N, BLOCK)
    mean = exchanged(mean, BLK).reshape(BLOCK, BLOCK)

    messages, ret = pl.pallas_call(
        block_kernel,
        out_shape=(
            jax.ShapeDtypeStruct((SIZES[0] * N, 16, BLOCK + LANES), BF16),
            jax.ShapeDtypeStruct((3 * ROWS, BLOCK), BF16),
        ),
        in_specs=[pl.BlockSpec(memory_space=pltpu.SMEM)] + vmem(2),
        out_specs=tuple(vmem(2)),
        scratch_shapes=[
            pltpu.VMEM((2, BLOCK, BLOCK), F32),
            pltpu.VMEM((2, BLOCK, BLOCK), BF16),
            pltpu.VMEM((2, BLOCK, BLOCK), BF16),
            pltpu.VMEM((2, BLOCK, BLOCK), F32),
            pltpu.VMEM((2, BLOCK, BLOCK), BF16),
            pltpu.VMEM((BLOCK, BLOCK), BF16),
            pltpu.VMEM((BLOCK, BLOCK), F32),
            pltpu.VMEM((BLOCK, BLOCK), BF16),
            pltpu.VMEM((BLOCK, BLOCK), BF16),
        ],
        compiler_params=pltpu.CompilerParams(vmem_limit_bytes=32 * 1024 * 1024),
        cost_estimate=pl.CostEstimate(flops=28 * 2 * BLOCK**3, bytes_accessed=4 << 20, transcendentals=0),
        name="block_update",
    )(y.astype(jnp.int32).reshape(1), mean, side)

    ret = lax.ppermute(ret, ALL, rep_with_y())
    got = exchanged(messages, FAN)
    got = exchanged(jnp.broadcast_to(got[None], (2, *got.shape)), "co")

    params, moment_rows = pl.pallas_call(
        final_kernel,
        out_shape=(
            jax.ShapeDtypeStruct((N, N, N * BLOCK), BF16),
            jax.ShapeDtypeStruct((ROWS, BLOCK), F32),
        ),
        in_specs=vmem(3),
        out_specs=tuple(vmem(2)),
        scratch_shapes=[pltpu.VMEM((2, WIDE, ROWS, LANES), F32)],
        compiler_params=pltpu.CompilerParams(vmem_limit_bytes=16 * 1024 * 1024),
        name="weights",
    )(got.reshape(2, SIZES[0] * N, 16, BLOCK + LANES), ret, momentum[0])
    left_next = stat_decay * left_stat[0] + (1.0 - stat_decay) * ret[ROWS : 2 * ROWS].astype(F32)
    right_next = stat_decay * right_stat[0] + (1.0 - stat_decay) * ret[2 * ROWS :].astype(F32)
    return (params, moment_rows[None], left_next[None], right_next[None])


def solution(mesh):
    split = Mesh(mesh.devices.reshape(SIZES), ALL)
    in_specs = (P(REP, BLK, None, None),) + (P(BLK, REP, None),) * 4
    out_specs = (P(BLK, None, None),) + (P(BLK, REP, None),) * 3
    return jax.shard_map(
        on_device, mesh=split, in_specs=in_specs, out_specs=out_specs, check_vma=False
    )
```

```python
import jax
import jax.numpy as jnp
from jax import lax
from jax.experimental import pallas as pl
from jax.experimental.pallas import tpu as pltpu
from jax.sharding import Mesh
from jax.sharding import PartitionSpec as P

REP = ("zl", "co")
ALL = ("zl", "co", "zh", "x", "y")
BLK = ("zh", "x", "y")
PLANE = ("zh", "y")
SIZES = (4, 2, 2, 4, 8)
N = 8
ROWS = 64
BLOCK = 512
ITERS = 4
LANES = 128
HALF = BLOCK // 2
SHARE = 3 * ROWS
MESSAGE = 40
WIDE = BLOCK // LANES

stat_decay = 0.9
moment_decay = 0.9
step_size = 0.25

F32 = jnp.float32
BF16 = jnp.bfloat16


def exchanged(pieces, axis):
    return lax.all_to_all(pieces, axis, split_axis=0, concat_axis=0, tiled=True)


def moved(shard, move):
    sizes = SIZES

    def place(where):
        index = 0
        for size, value in zip(sizes, where):
            index = index * size + value
        return index

    def device(index):
        where = []
        for size in reversed(sizes):
            where.append(index % size)
            index //= size
        return tuple(reversed(where))

    count = 1
    for size in sizes:
        count *= size
    pairs = [(k, place(move(*device(k)))) for k in range(count)]
    return lax.ppermute(shard, ALL, pairs)


def turned(shard):
    return moved(shard, lambda zl, co, zh, x, y: (x, co, zh, zl, y))


def along_x(shard, flip):
    return moved(shard, lambda zl, co, zh, x, y: (zl, co, zh, x ^ flip, y))


def other_core(shard):
    return moved(shard, lambda zl, co, zh, x, y: (zl, 1 - co, zh, x, y))


def spread(shard, axis):
    copies = jnp.broadcast_to(shard[None], (lax.axis_size(axis), *shard.shape))
    return exchanged(copies, axis)


def three_parts(value):
    high = value.astype(BF16).astype(F32)
    rest = value - high
    middle = rest.astype(BF16).astype(F32)
    return high, middle, rest - middle


def dot(a, b, dims=((1,), (0,))):
    return lax.dot_general(a, b, (dims, ((), ())), preferred_element_type=F32)


def pack_kernel(grad_ref, out_ref, rows_f):
    for j in range(N):
        for w in range(WIDE):
            slot = (j * WIDE + w) % 4
            for p in range(N):
                cols = slice(j * BLOCK + w * LANES, j * BLOCK + (w + 1) * LANES)
                rows_f[slot, p * N : (p + 1) * N, :] = grad_ref[p, :, cols].astype(F32)
            lanes = slice(w % 2 * LANES, (w % 2 + 1) * LANES)
            for i in range(N):
                at = (i // 4 * N + j) * N
                rows = rows_f[slot, pl.ds(i, N, stride=N), :]
                out_ref[i % 4 * 2 + w // 2, at : at + N, lanes] = rows.astype(BF16)


def gram_kernel(own_ref, got_ref, g_ref, gram_ref, ret_ref, g_b):
    own = pl.multiple_of(own_ref[0] * ROWS, ROWS)
    for half in range(2):
        for x in range(4):
            for zh in range(2):
                rows = slice((zh * 4 + x) * ROWS, (zh * 4 + x + 1) * ROWS)
                part = got_ref[half, (x * 2 + zh) * ROWS : (x * 2 + zh + 1) * ROWS, :]
                cols = slice(half * HALF, (half + 1) * HALF)
                g_ref[rows, cols] = part
                g_b[rows, cols] = part.astype(BF16)
    for side in range(2):
        gram_ref[side] = dot(g_b[...], g_b[...], (((1,), (1,)), ((0,), (0,)))[side])
        ret_ref[side * ROWS : (side + 1) * ROWS, :] = gram_ref[side, pl.ds(own, ROWS), :].astype(BF16)


def block_kernel(
    own_ref, g_ref, gram_ref, s0_ref, s1_ref, s2_ref, s3_ref, twin_ref,
    msg_ref, ret_ref, m_f, m_b, v_b, w_f, w_b, y_f, y_b, z_b, base_f,
):
    own = pl.multiple_of(own_ref[0] * ROWS, ROWS)
    x = own_ref[0] >> 1
    co = own_ref[0] & 1
    chunk = BLOCK // 2
    spans = [pl.ds(k * chunk, chunk) for k in range(2)]
    norm_g = jnp.zeros((1, 1), F32)
    for rows in spans:
        part = g_ref[rows, :]
        norm_g += jnp.sum(part * part, keepdims=True)
        y_f[rows, :] = part
        y_b[rows, :] = part.astype(BF16)
    shares = []
    for flip, ref in enumerate((s0_ref, s1_ref, s2_ref, s3_ref)):
        shares.append((pl.multiple_of((own_ref[0] ^ (2 * flip)) * ROWS, ROWS), ref, 0))
        shares.append((pl.multiple_of((own_ref[0] ^ (2 * flip + 1)) * ROWS, ROWS), twin_ref, flip * SHARE))
    scale = jnp.ones((1, 1), F32)
    for side in range(2):
        total = jnp.zeros((1, 1), F32)
        for at, ref, start in shares:
            rows = pl.ds(at, ROWS)
            old = ref[start + side * ROWS : start + (side + 1) * ROWS, :].astype(F32)
            new = stat_decay * old + (1.0 - stat_decay) * gram_ref[side, rows, :]
            m_f[side, rows, :] = new
            total += jnp.sum(new * new, keepdims=True)
        frob = jnp.sqrt(total)
        scale = scale / jnp.sqrt(jnp.sqrt(frob))
        inverse = 1.0 / frob
        for rows in spans:
            new = m_f[side, rows, :] * inverse
            m_f[side, rows, :] = new
            m_b[side, rows, :] = new.astype(BF16)
    for at, ref, start in shares:
        base_f[pl.ds(at, ROWS), :] = ref[start + 2 * ROWS : start + 3 * ROWS, :].astype(F32)

    def apply_factors():
        for rows in spans:
            new = 1.25 * y_f[rows, :] - 0.25 * dot(m_b[0, rows, :], y_b[...])
            y_f[rows, :] = new
            z_b[rows, :] = new.astype(BF16)
        for rows in spans:
            new = 1.25 * y_f[rows, :] - 0.25 * dot(z_b[rows, :], m_b[1])
            y_f[rows, :] = new
            y_b[rows, :] = new.astype(BF16)

    def sweep(_, carry):
        for side in range(2):
            for rows in spans:
                square = dot(m_b[side, rows, :], m_b[side])
                v_b[side, rows, :] = (0.0625 * square - 0.625 * m_f[side, rows, :]).astype(BF16)
        apply_factors()
        for side in range(2):
            for rows in spans:
                new = 1.5625 * m_f[side, rows, :] + dot(v_b[side, rows, :], m_b[side])
                w_f[side, rows, :] = new
                w_b[side, rows, :] = new.astype(BF16)
        for side in range(2):
            for rows in spans:
                new = 1.5625 * w_f[side, rows, :] + dot(v_b[side, rows, :], w_b[side])
                m_f[side, rows, :] = new
                m_b[side, rows, :] = new.astype(BF16)
        return carry

    lax.fori_loop(0, ITERS - 1, sweep, 0)
    apply_factors()
    norm_p = jnp.zeros((1, 1), F32)
    for rows in spans:
        new = y_f[rows, :] * scale
        norm_p += jnp.sum(new * new, keepdims=True)
        y_f[rows, :] = new
    ret_ref[...] = y_f[pl.ds(own, ROWS), :].astype(BF16)
    lane = lax.broadcasted_iota(jnp.int32, (N, LANES), 1)
    norms = jnp.zeros((N, LANES), F32)
    for k, part in enumerate(three_parts(norm_p) + three_parts(norm_g)):
        norms = jnp.where(lane == k, part, norms)
    norms = norms.astype(BF16)
    for zh in range(2):
        for row in range(N):
            rows = pl.ds(pl.multiple_of((zh * 4 + x) * ROWS + row * N, N), N)
            for k, ref in enumerate((y_f, base_f)):
                whole = ref[rows, :]
                half = jnp.where(co == 0, whole[:, :HALF], whole[:, HALF:])
                both = jnp.concatenate([half[:, :LANES], half[:, LANES:]], axis=0)
                msg_ref[zh * N + row, k * 2 * N : (k + 1) * 2 * N, :] = both.astype(BF16)
            msg_ref[zh * N + row, 4 * N : 5 * N, :] = norms


def weight_kernel(got_ref, ret_ref, mom_ref, half_ref, mom_out_ref, rows_f):
    total = jnp.zeros((N, LANES), F32)
    for z in range(4):
        for k in range(2 * N):
            total += got_ref[z, k, 4 * N : 5 * N, :].astype(F32)
    lane = lax.broadcasted_iota(jnp.int32, (N, LANES), 1)
    norm_p = jnp.sum(jnp.where(lane < 3, total, 0.0), keepdims=True) * (1.0 / N)
    norm_g = jnp.sum(jnp.where(lane < 3, 0.0, total), keepdims=True) * (1.0 / N)
    graft = jnp.sqrt(norm_g) / jnp.sqrt(norm_p)
    for j in range(N):
        slot = j % 2
        for zh in range(2):
            for z in range(4):
                i = zh * 4 + z
                precond = got_ref[z, zh * N + j, 0 : 2 * N, :].astype(F32)
                base = got_ref[z, zh * N + j, 2 * N : 4 * N, :].astype(F32)
                new = base - step_size * (graft * precond)
                for w in range(2):
                    rows_f[slot, w, i * N : (i + 1) * N, :] = new[w * N : (w + 1) * N, :]
        for p in range(N):
            for w in range(2):
                cols = slice(j * HALF + w * LANES, j * HALF + (w + 1) * LANES)
                half_ref[p, :, cols] = rows_f[slot, w, pl.ds(p, N, stride=N), :].astype(BF16)
    mom_out_ref[...] = moment_decay * mom_ref[...] + graft * ret_ref[...].astype(F32)


def join_kernel(got_ref, out_ref):
    for p in range(N):
        for j in range(N):
            for h in range(2):
                cols = slice(j * BLOCK + h * HALF, j * BLOCK + (h + 1) * HALF)
                out_ref[p, :, cols] = got_ref[h, p, :, j * HALF : (j + 1) * HALF]


def vmem(count):
    return [pl.BlockSpec(memory_space=pltpu.VMEM)] * count


def scratch(*shape, dtype):
    return pltpu.VMEM(shape, dtype)


def call(kernel, outs, scratches, flops=0, scalars=0, arrays=1, mib=32):
    return pl.pallas_call(
        kernel,
        out_shape=tuple(jax.ShapeDtypeStruct(*o) for o in outs),
        in_specs=[pl.BlockSpec(memory_space=pltpu.SMEM)] * scalars + vmem(arrays),
        out_specs=tuple(vmem(len(outs))),
        scratch_shapes=scratches,
        compiler_params=pltpu.CompilerParams(vmem_limit_bytes=mib * 1024 * 1024),
        cost_estimate=pl.CostEstimate(flops=flops, bytes_accessed=1 << 20, transcendentals=0),
    )


def step(gradients, left_stat, right_stat, momentum, master):
    own = (lax.axis_index("x") * 2 + lax.axis_index("co")).astype(jnp.int32).reshape(1)
    base = master[0] - (step_size * moment_decay) * momentum[0]
    share = jnp.concatenate([a.astype(BF16) for a in (left_stat[0], right_stat[0], base)], axis=0)
    s0 = turned(share)
    shares = [s0] + [along_x(s0, flip) for flip in (1, 2, 3)]
    twin = other_core(jnp.concatenate(shares, axis=0))

    (pieces,) = call(
        pack_kernel, [((N, 2 * ROWS, HALF), BF16)], [scratch(4, ROWS, LANES, dtype=F32)], mib=8
    )(gradients[0])
    pieces = exchanged(pieces, REP)
    mean = jnp.sum(pieces.astype(F32), axis=0) * (1.0 / N)
    mean = exchanged(mean.reshape(2 * N, N, HALF), PLANE)
    mean = spread(mean.reshape(2 * ROWS, HALF), "x")
    mean = spread(mean.reshape(BLOCK, HALF), "co")

    mean, grams, ret = call(
        gram_kernel,
        [((BLOCK, BLOCK), F32), ((2, BLOCK, BLOCK), F32), ((2 * ROWS, BLOCK), BF16)],
        [scratch(BLOCK, BLOCK, dtype=BF16)],
        flops=4 * BLOCK**3,
        scalars=1,
        mib=16,
    )(own, mean)
    ret = turned(ret)
    update = call(
        block_kernel,
        [((2 * N, MESSAGE, LANES), BF16), ((ROWS, BLOCK), BF16)],
        [
            scratch(2, BLOCK, BLOCK, dtype=F32),
            scratch(2, BLOCK, BLOCK, dtype=BF16),
            scratch(2, BLOCK, BLOCK, dtype=BF16),
            scratch(2, BLOCK, BLOCK, dtype=F32),
            scratch(2, BLOCK, BLOCK, dtype=BF16),
            scratch(BLOCK, BLOCK, dtype=F32),
            scratch(BLOCK, BLOCK, dtype=BF16),
            scratch(BLOCK, BLOCK, dtype=BF16),
            scratch(BLOCK, BLOCK, dtype=F32),
        ],
        flops=52 * BLOCK**3,
        scalars=1,
        arrays=7,
    )
    messages, rows = update(own, mean, grams, *shares, twin)
    rows = turned(rows)
    got = exchanged(messages, PLANE)
    got = spread(got, "zl")
    half, moment_rows = call(
        weight_kernel,
        [((N, N, N * HALF), BF16), ((ROWS, BLOCK), F32)],
        [scratch(2, 2, ROWS, LANES, dtype=F32)],
        arrays=3,
        mib=16,
    )(got, rows, momentum[0])
    half = spread(half, "co")
    (params,) = call(join_kernel, [((N, N, N * BLOCK), BF16)], [], mib=8)(half)
    left_next = stat_decay * left_stat[0] + (1.0 - stat_decay) * ret[:ROWS].astype(F32)
    right_next = stat_decay * right_stat[0] + (1.0 - stat_decay) * ret[ROWS:].astype(F32)
    return (params, moment_rows[None], left_next[None], right_next[None])


def solution(mesh):
    split = Mesh(mesh.devices.reshape(SIZES), ALL)
    in_specs = (P(REP, BLK, None, None),) + (P(BLK, REP, None),) * 4
    out_specs = (P(BLK, None, None),) + (P(BLK, REP, None),) * 3
    return jax.shard_map(step, mesh=split, in_specs=in_specs, out_specs=out_specs, check_vma=False)
```

```python
import jax
import jax.numpy as jnp
from jax import lax
from jax.experimental import pallas as pl
from jax.experimental.pallas import tpu as pltpu
from jax.sharding import Mesh
from jax.sharding import PartitionSpec as P

REP = ("zl", "co")
ALL = ("zl", "co", "zh", "x", "y")
BLK = ("zh", "x", "y")
PLANE = ("zh", "y")
SOLID = ("zl", "zh", "y")
SIZES = (4, 2, 2, 4, 8)
N = 8
ROWS = 64
BLOCK = 512
ITERS = 4
LANES = 128
HALF = BLOCK // 2
SHARE = 3 * ROWS
MESSAGE = 40
WIDE = BLOCK // LANES

stat_decay = 0.9
moment_decay = 0.9
step_size = 0.25

F32 = jnp.float32
BF16 = jnp.bfloat16


def exchanged(pieces, axis):
    return lax.all_to_all(pieces, axis, split_axis=0, concat_axis=0, tiled=True)


def moved(shard, move):
    sizes = SIZES

    def place(where):
        index = 0
        for size, value in zip(sizes, where):
            index = index * size + value
        return index

    def device(index):
        where = []
        for size in reversed(sizes):
            where.append(index % size)
            index //= size
        return tuple(reversed(where))

    count = 1
    for size in sizes:
        count *= size
    pairs = [(k, place(move(*device(k)))) for k in range(count)]
    return lax.ppermute(shard, ALL, pairs)


def turned(shard):
    return moved(shard, lambda zl, co, zh, x, y: (x, co, zh, zl, y))


def along_x(shard, flip):
    return moved(shard, lambda zl, co, zh, x, y: (zl, co, zh, x ^ flip, y))


def other_core(shard):
    return moved(shard, lambda zl, co, zh, x, y: (zl, 1 - co, zh, x, y))


def spread(shard, axis):
    copies = jnp.broadcast_to(shard[None], (lax.axis_size(axis), *shard.shape))
    return exchanged(copies, axis)


def three_parts(value):
    high = value.astype(BF16).astype(F32)
    rest = value - high
    middle = rest.astype(BF16).astype(F32)
    return high, middle, rest - middle


def dot(a, b, dims=((1,), (0,))):
    return lax.dot_general(a, b, (dims, ((), ())), preferred_element_type=F32)


def pack_kernel(grad_ref, out_ref, rows_f):
    for j in range(N):
        for w in range(WIDE):
            slot = (j * WIDE + w) % 4
            for p in range(N):
                cols = slice(j * BLOCK + w * LANES, j * BLOCK + (w + 1) * LANES)
                rows_f[slot, p * N : (p + 1) * N, :] = grad_ref[p, :, cols].astype(F32)
            lanes = slice(w % 2 * LANES, (w % 2 + 1) * LANES)
            for i in range(N):
                at = (i // 4 * N + j) * N
                rows = rows_f[slot, pl.ds(i, N, stride=N), :]
                out_ref[i % 4 * 2 + w // 2, at : at + N, lanes] = rows.astype(BF16)


def gram_kernel(own_ref, got_ref, g_ref, gram_ref, ret_ref, g_b):
    own = pl.multiple_of(own_ref[0] * ROWS, ROWS)
    for half in range(2):
        for x in range(4):
            for zh in range(2):
                rows = slice((zh * 4 + x) * ROWS, (zh * 4 + x + 1) * ROWS)
                part = got_ref[half, (x * 2 + zh) * ROWS : (x * 2 + zh + 1) * ROWS, :]
                cols = slice(half * HALF, (half + 1) * HALF)
                g_ref[rows, cols] = part
                g_b[rows, cols] = part.astype(BF16)
    for side in range(2):
        gram_ref[side] = dot(g_b[...], g_b[...], (((1,), (1,)), ((0,), (0,)))[side])
        ret_ref[side * ROWS : (side + 1) * ROWS, :] = gram_ref[side, pl.ds(own, ROWS), :].astype(BF16)


def block_kernel(
    own_ref, g_ref, gram_ref, s0_ref, s1_ref, s2_ref, s3_ref, twin_ref,
    msg_ref, ret_ref, m_f, m_b, v_b, w_f, w_b, y_f, y_b, z_b, base_f,
):
    own = pl.multiple_of(own_ref[0] * ROWS, ROWS)
    x = own_ref[0] >> 1
    co = own_ref[0] & 1
    chunk = BLOCK // 2
    spans = [pl.ds(k * chunk, chunk) for k in range(2)]
    norm_g = jnp.zeros((1, 1), F32)
    for rows in spans:
        part = g_ref[rows, :]
        norm_g += jnp.sum(part * part, keepdims=True)
        y_f[rows, :] = part
        y_b[rows, :] = part.astype(BF16)
    shares = []
    for flip, ref in enumerate((s0_ref, s1_ref, s2_ref, s3_ref)):
        shares.append((pl.multiple_of((own_ref[0] ^ (2 * flip)) * ROWS, ROWS), ref, 0))
        shares.append((pl.multiple_of((own_ref[0] ^ (2 * flip + 1)) * ROWS, ROWS), twin_ref, flip * SHARE))
    scale = jnp.ones((1, 1), F32)
    for side in range(2):
        total = jnp.zeros((1, 1), F32)
        for at, ref, start in shares:
            rows = pl.ds(at, ROWS)
            old = ref[start + side * ROWS : start + (side + 1) * ROWS, :].astype(F32)
            new = stat_decay * old + (1.0 - stat_decay) * gram_ref[side, rows, :]
            m_f[side, rows, :] = new
            total += jnp.sum(new * new, keepdims=True)
        frob = jnp.sqrt(total)
        scale = scale / jnp.sqrt(jnp.sqrt(frob))
        inverse = 1.0 / frob
        for rows in spans:
            new = m_f[side, rows, :] * inverse
            m_f[side, rows, :] = new
            m_b[side, rows, :] = new.astype(BF16)
    for at, ref, start in shares:
        base_f[pl.ds(at, ROWS), :] = ref[start + 2 * ROWS : start + 3 * ROWS, :].astype(F32)

    def apply_factors():
        for rows in spans:
            new = 1.25 * y_f[rows, :] - 0.25 * dot(m_b[0, rows, :], y_b[...])
            y_f[rows, :] = new
            z_b[rows, :] = new.astype(BF16)
        for rows in spans:
            new = 1.25 * y_f[rows, :] - 0.25 * dot(z_b[rows, :], m_b[1])
            y_f[rows, :] = new
            y_b[rows, :] = new.astype(BF16)

    def sweep(_, carry):
        for side in range(2):
            for rows in spans:
                square = dot(m_b[side, rows, :], m_b[side])
                v_b[side, rows, :] = (0.0625 * square - 0.625 * m_f[side, rows, :]).astype(BF16)
        apply_factors()
        for side in range(2):
            for rows in spans:
                new = 1.5625 * m_f[side, rows, :] + dot(v_b[side, rows, :], m_b[side])
                w_f[side, rows, :] = new
                w_b[side, rows, :] = new.astype(BF16)
        for side in range(2):
            for rows in spans:
                new = 1.5625 * w_f[side, rows, :] + dot(v_b[side, rows, :], w_b[side])
                m_f[side, rows, :] = new
                m_b[side, rows, :] = new.astype(BF16)
        return carry

    lax.fori_loop(0, ITERS - 1, sweep, 0)
    apply_factors()
    norm_p = jnp.zeros((1, 1), F32)
    for rows in spans:
        new = y_f[rows, :] * scale
        norm_p += jnp.sum(new * new, keepdims=True)
        y_f[rows, :] = new
    ret_ref[...] = y_f[pl.ds(own, ROWS), :].astype(BF16)
    lane = lax.broadcasted_iota(jnp.int32, (N, LANES), 1)
    norms = jnp.zeros((N, LANES), F32)
    for k, part in enumerate(three_parts(norm_p) + three_parts(norm_g)):
        norms = jnp.where(lane == k, part, norms)
    norms = norms.astype(BF16)
    for zh in range(2):
        for row in range(N):
            rows = pl.ds(pl.multiple_of((zh * 4 + x) * ROWS + row * N, N), N)
            for k, ref in enumerate((y_f, base_f)):
                whole = ref[rows, :]
                half = jnp.where(co == 0, whole[:, :HALF], whole[:, HALF:])
                both = jnp.concatenate([half[:, :LANES], half[:, LANES:]], axis=0)
                both = both.astype(BF16)
                for z in range(4):
                    at = (z * 2 + zh) * N + row
                    msg_ref[at, k * 2 * N : (k + 1) * 2 * N, :] = both
            for z in range(4):
                msg_ref[(z * 2 + zh) * N + row, 4 * N : 5 * N, :] = norms


def weight_kernel(got_ref, ret_ref, mom_ref, half_ref, mom_out_ref, rows_f):
    total = jnp.zeros((N, LANES), F32)
    for k in range(8 * N):
        total += got_ref[k, 4 * N : 5 * N, :].astype(F32)
    lane = lax.broadcasted_iota(jnp.int32, (N, LANES), 1)
    norm_p = jnp.sum(jnp.where(lane < 3, total, 0.0), keepdims=True) * (1.0 / N)
    norm_g = jnp.sum(jnp.where(lane < 3, 0.0, total), keepdims=True) * (1.0 / N)
    graft = jnp.sqrt(norm_g) / jnp.sqrt(norm_p)
    for j in range(N):
        slot = j % 2
        for zh in range(2):
            for z in range(4):
                i = zh * 4 + z
                at = (z * 2 + zh) * N + j
                precond = got_ref[at, 0 : 2 * N, :].astype(F32)
                base = got_ref[at, 2 * N : 4 * N, :].astype(F32)
                new = base - step_size * (graft * precond)
                for w in range(2):
                    rows_f[slot, w, i * N : (i + 1) * N, :] = new[w * N : (w + 1) * N, :]
        for p in range(N):
            for w in range(2):
                cols = slice(j * HALF + w * LANES, j * HALF + (w + 1) * LANES)
                half_ref[p, :, cols] = rows_f[slot, w, pl.ds(p, N, stride=N), :].astype(BF16)
    mom_out_ref[...] = moment_decay * mom_ref[...] + graft * ret_ref[...].astype(F32)


def join_kernel(got_ref, out_ref):
    for p in range(N):
        for j in range(N):
            for h in range(2):
                cols = slice(j * BLOCK + h * HALF, j * BLOCK + (h + 1) * HALF)
                out_ref[p, :, cols] = got_ref[h, p, :, j * HALF : (j + 1) * HALF]


def vmem(count):
    return [pl.BlockSpec(memory_space=pltpu.VMEM)] * count


def scratch(*shape, dtype):
    return pltpu.VMEM(shape, dtype)


def call(kernel, outs, scratches, flops=0, scalars=0, arrays=1, mib=32):
    return pl.pallas_call(
        kernel,
        out_shape=tuple(jax.ShapeDtypeStruct(*o) for o in outs),
        in_specs=[pl.BlockSpec(memory_space=pltpu.SMEM)] * scalars + vmem(arrays),
        out_specs=tuple(vmem(len(outs))),
        scratch_shapes=scratches,
        compiler_params=pltpu.CompilerParams(vmem_limit_bytes=mib * 1024 * 1024),
        cost_estimate=pl.CostEstimate(flops=flops, bytes_accessed=1 << 20, transcendentals=0),
    )


def step(gradients, left_stat, right_stat, momentum, master):
    own = (lax.axis_index("x") * 2 + lax.axis_index("co")).astype(jnp.int32).reshape(1)
    base = master[0] - (step_size * moment_decay) * momentum[0]
    share = jnp.concatenate([a.astype(BF16) for a in (left_stat[0], right_stat[0], base)], axis=0)
    s0 = turned(share)
    shares = [s0] + [along_x(s0, flip) for flip in (1, 2, 3)]
    twin = other_core(jnp.concatenate(shares, axis=0))

    (pieces,) = call(
        pack_kernel, [((N, 2 * ROWS, HALF), BF16)], [scratch(4, ROWS, LANES, dtype=F32)], mib=8
    )(gradients[0])
    pieces = exchanged(pieces, REP)
    mean = jnp.sum(pieces.astype(F32), axis=0) * (1.0 / N)
    mean = exchanged(mean.reshape(2 * N, N, HALF), PLANE)
    mean = spread(mean.reshape(2 * ROWS, HALF), "x")
    mean = spread(mean.reshape(BLOCK, HALF), "co")

    mean, grams, ret = call(
        gram_kernel,
        [((BLOCK, BLOCK), F32), ((2, BLOCK, BLOCK), F32), ((2 * ROWS, BLOCK), BF16)],
        [scratch(BLOCK, BLOCK, dtype=BF16)],
        flops=4 * BLOCK**3,
        scalars=1,
        mib=16,
    )(own, mean)
    ret = turned(ret)
    update = call(
        block_kernel,
        [((8 * N, MESSAGE, LANES), BF16), ((ROWS, BLOCK), BF16)],
        [
            scratch(2, BLOCK, BLOCK, dtype=F32),
            scratch(2, BLOCK, BLOCK, dtype=BF16),
            scratch(2, BLOCK, BLOCK, dtype=BF16),
            scratch(2, BLOCK, BLOCK, dtype=F32),
            scratch(2, BLOCK, BLOCK, dtype=BF16),
            scratch(BLOCK, BLOCK, dtype=F32),
            scratch(BLOCK, BLOCK, dtype=BF16),
            scratch(BLOCK, BLOCK, dtype=BF16),
            scratch(BLOCK, BLOCK, dtype=F32),
        ],
        flops=52 * BLOCK**3,
        scalars=1,
        arrays=7,
    )
    messages, rows = update(own, mean, grams, *shares, twin)
    rows = turned(rows)
    got = exchanged(messages, SOLID)
    half, moment_rows = call(
        weight_kernel,
        [((N, N, N * HALF), BF16), ((ROWS, BLOCK), F32)],
        [scratch(2, 2, ROWS, LANES, dtype=F32)],
        arrays=3,
        mib=16,
    )(got, rows, momentum[0])
    half = spread(half, "co")
    (params,) = call(join_kernel, [((N, N, N * BLOCK), BF16)], [], mib=8)(half)
    left_next = stat_decay * left_stat[0] + (1.0 - stat_decay) * ret[:ROWS].astype(F32)
    right_next = stat_decay * right_stat[0] + (1.0 - stat_decay) * ret[ROWS:].astype(F32)
    return (params, moment_rows[None], left_next[None], right_next[None])


def solution(mesh):
    split = Mesh(mesh.devices.reshape(SIZES), ALL)
    in_specs = (P(REP, BLK, None, None),) + (P(BLK, REP, None),) * 4
    out_specs = (P(BLK, None, None),) + (P(BLK, REP, None),) * 3
    return jax.shard_map(step, mesh=split, in_specs=in_specs, out_specs=out_specs, check_vma=False)
```

```python
import jax
import jax.numpy as jnp
from jax import lax
from jax.experimental import pallas as pl
from jax.experimental.pallas import tpu as pltpu
from jax.sharding import Mesh
from jax.sharding import PartitionSpec as P

REP = ("zl", "co")
ALL = ("zl", "co", "zh", "x", "y")
BLK = ("zh", "x", "y")
PLANE = ("zh", "y")
SOLID = ("zl", "zh", "y")
SIZES = (4, 2, 2, 4, 8)
N = 8
ROWS = 64
BLOCK = 512
ITERS = 4
LANES = 128
HALF = BLOCK // 2
SHARE = 3 * ROWS
MESSAGE = 40
WIDE = BLOCK // LANES

stat_decay = 0.9
moment_decay = 0.9
step_size = 0.25

F32 = jnp.float32
BF16 = jnp.bfloat16


def exchanged(pieces, axis):
    return lax.all_to_all(pieces, axis, split_axis=0, concat_axis=0, tiled=True)


def moved(shard, move):
    sizes = SIZES

    def place(where):
        index = 0
        for size, value in zip(sizes, where):
            index = index * size + value
        return index

    def device(index):
        where = []
        for size in reversed(sizes):
            where.append(index % size)
            index //= size
        return tuple(reversed(where))

    count = 1
    for size in sizes:
        count *= size
    pairs = [(k, place(move(*device(k)))) for k in range(count)]
    return lax.ppermute(shard, ALL, pairs)


def turned(shard):
    return moved(shard, lambda zl, co, zh, x, y: (x, co, zh, zl, y))


def along_x(shard, flip):
    return moved(shard, lambda zl, co, zh, x, y: (zl, co, zh, x ^ flip, y))


def other_core(shard):
    return moved(shard, lambda zl, co, zh, x, y: (zl, 1 - co, zh, x, y))


def spread(shard, axis):
    copies = jnp.broadcast_to(shard[None], (lax.axis_size(axis), *shard.shape))
    return exchanged(copies, axis)


def three_parts(value):
    high = value.astype(BF16).astype(F32)
    rest = value - high
    middle = rest.astype(BF16).astype(F32)
    return high, middle, rest - middle


def dot(a, b, dims=((1,), (0,))):
    return lax.dot_general(a, b, (dims, ((), ())), preferred_element_type=F32)


def pack_kernel(
    grad_hbm, left_hbm, right_hbm, mom_hbm, master_hbm,
    out_ref, share_ref, grad_ref, rows_f, state_f, grad_sem, state_sem,
):
    loads = []
    for j in range(N):
        cols = pl.ds(j * BLOCK, BLOCK)
        load = pltpu.make_async_copy(grad_hbm.at[:, :, cols], grad_ref.at[:, :, cols], grad_sem.at[j])
        load.start()
        loads.append(load)
    states = []
    for k, ref in enumerate((left_hbm, right_hbm, mom_hbm, master_hbm)):
        load = pltpu.make_async_copy(ref, state_f.at[k], state_sem.at[k])
        load.start()
        states.append(load)
    for j in range(N):
        loads[j].wait()
        for w in range(WIDE):
            slot = (j * WIDE + w) % 4
            for p in range(N):
                cols = slice(j * BLOCK + w * LANES, j * BLOCK + (w + 1) * LANES)
                rows_f[slot, p * N : (p + 1) * N, :] = grad_ref[p, :, cols].astype(F32)
            lanes = slice(w % 2 * LANES, (w % 2 + 1) * LANES)
            for i in range(N):
                at = (i // 4 * N + j) * N
                rows = rows_f[slot, pl.ds(i, N, stride=N), :]
                out_ref[i % 4 * 2 + w // 2, at : at + N, lanes] = rows.astype(BF16)
    for load in states:
        load.wait()
    share_ref[0:ROWS, :] = state_f[0].astype(BF16)
    share_ref[ROWS : 2 * ROWS, :] = state_f[1].astype(BF16)
    base = state_f[3] - (step_size * moment_decay) * state_f[2]
    share_ref[2 * ROWS : 3 * ROWS, :] = base.astype(BF16)


def gram_kernel(own_ref, got_ref, g_ref, gram_ref, ret_ref, g_b):
    own = pl.multiple_of(own_ref[0] * ROWS, ROWS)
    for half in range(2):
        for x in range(4):
            for zh in range(2):
                rows = slice((zh * 4 + x) * ROWS, (zh * 4 + x + 1) * ROWS)
                part = got_ref[half, (x * 2 + zh) * ROWS : (x * 2 + zh + 1) * ROWS, :]
                cols = slice(half * HALF, (half + 1) * HALF)
                g_ref[rows, cols] = part
                g_b[rows, cols] = part.astype(BF16)
    for side in range(2):
        gram_ref[side] = dot(g_b[...], g_b[...], (((1,), (1,)), ((0,), (0,)))[side])
        ret_ref[side * ROWS : (side + 1) * ROWS, :] = gram_ref[side, pl.ds(own, ROWS), :].astype(BF16)


def block_kernel(
    own_ref, g_ref, gram_ref, s0_ref, s1_ref, s2_ref, s3_ref, twin_ref,
    msg_ref, ret_ref, m_f, m_b, v_b, w_f, w_b, y_f, y_b, z_b, base_f,
):
    own = pl.multiple_of(own_ref[0] * ROWS, ROWS)
    x = own_ref[0] >> 1
    co = own_ref[0] & 1
    chunk = BLOCK // 2
    spans = [pl.ds(k * chunk, chunk) for k in range(2)]
    norm_g = jnp.zeros((1, 1), F32)
    for rows in spans:
        part = g_ref[rows, :]
        norm_g += jnp.sum(part * part, keepdims=True)
        y_f[rows, :] = part
        y_b[rows, :] = part.astype(BF16)
    shares = []
    for flip, ref in enumerate((s0_ref, s1_ref, s2_ref, s3_ref)):
        shares.append((pl.multiple_of((own_ref[0] ^ (2 * flip)) * ROWS, ROWS), ref, 0))
        shares.append((pl.multiple_of((own_ref[0] ^ (2 * flip + 1)) * ROWS, ROWS), twin_ref, flip * SHARE))
    scale = jnp.ones((1, 1), F32)
    for side in range(2):
        total = jnp.zeros((1, 1), F32)
        for at, ref, start in shares:
            rows = pl.ds(at, ROWS)
            old = ref[start + side * ROWS : start + (side + 1) * ROWS, :].astype(F32)
            new = stat_decay * old + (1.0 - stat_decay) * gram_ref[side, rows, :]
            m_f[side, rows, :] = new
            total += jnp.sum(new * new, keepdims=True)
        frob = jnp.sqrt(total)
        scale = scale / jnp.sqrt(jnp.sqrt(frob))
        inverse = 1.0 / frob
        for rows in spans:
            new = m_f[side, rows, :] * inverse
            m_f[side, rows, :] = new
            m_b[side, rows, :] = new.astype(BF16)
    for at, ref, start in shares:
        base_f[pl.ds(at, ROWS), :] = ref[start + 2 * ROWS : start + 3 * ROWS, :].astype(F32)

    def apply_factors():
        for rows in spans:
            new = 1.25 * y_f[rows, :] - 0.25 * dot(m_b[0, rows, :], y_b[...])
            y_f[rows, :] = new
            z_b[rows, :] = new.astype(BF16)
        for rows in spans:
            new = 1.25 * y_f[rows, :] - 0.25 * dot(z_b[rows, :], m_b[1])
            y_f[rows, :] = new
            y_b[rows, :] = new.astype(BF16)

    def sweep(_, carry):
        for side in range(2):
            for rows in spans:
                square = dot(m_b[side, rows, :], m_b[side])
                v_b[side, rows, :] = (0.0625 * square - 0.625 * m_f[side, rows, :]).astype(BF16)
        apply_factors()
        for side in range(2):
            for rows in spans:
                new = 1.5625 * m_f[side, rows, :] + dot(v_b[side, rows, :], m_b[side])
                w_f[side, rows, :] = new
                w_b[side, rows, :] = new.astype(BF16)
        for side in range(2):
            for rows in spans:
                new = 1.5625 * w_f[side, rows, :] + dot(v_b[side, rows, :], w_b[side])
                m_f[side, rows, :] = new
                m_b[side, rows, :] = new.astype(BF16)
        return carry

    lax.fori_loop(0, ITERS - 1, sweep, 0)
    apply_factors()
    norm_p = jnp.zeros((1, 1), F32)
    for rows in spans:
        new = y_f[rows, :] * scale
        norm_p += jnp.sum(new * new, keepdims=True)
        y_f[rows, :] = new
    ret_ref[...] = y_f[pl.ds(own, ROWS), :].astype(BF16)
    lane = lax.broadcasted_iota(jnp.int32, (N, LANES), 1)
    norms = jnp.zeros((N, LANES), F32)
    for k, part in enumerate(three_parts(norm_p) + three_parts(norm_g)):
        norms = jnp.where(lane == k, part, norms)
    norms = norms.astype(BF16)
    for zh in range(2):
        for row in range(N):
            rows = pl.ds(pl.multiple_of((zh * 4 + x) * ROWS + row * N, N), N)
            for k, ref in enumerate((y_f, base_f)):
                whole = ref[rows, :]
                half = jnp.where(co == 0, whole[:, :HALF], whole[:, HALF:])
                both = jnp.concatenate([half[:, :LANES], half[:, LANES:]], axis=0)
                both = both.astype(BF16)
                for z in range(4):
                    at = (z * 2 + zh) * N + row
                    msg_ref[at, k * 2 * N : (k + 1) * 2 * N, :] = both
            for z in range(4):
                msg_ref[(z * 2 + zh) * N + row, 4 * N : 5 * N, :] = norms


def weight_kernel(got_ref, half_ref, graft_ref, rows_f):
    total = jnp.zeros((N, LANES), F32)
    for k in range(8 * N):
        total += got_ref[k, 4 * N : 5 * N, :].astype(F32)
    lane = lax.broadcasted_iota(jnp.int32, (N, LANES), 1)
    norm_p = jnp.sum(jnp.where(lane < 3, total, 0.0), keepdims=True) * (1.0 / N)
    norm_g = jnp.sum(jnp.where(lane < 3, 0.0, total), keepdims=True) * (1.0 / N)
    graft = jnp.sqrt(norm_g) / jnp.sqrt(norm_p)
    for j in range(N):
        slot = j % 2
        for zh in range(2):
            for z in range(4):
                i = zh * 4 + z
                at = (z * 2 + zh) * N + j
                precond = got_ref[at, 0 : 2 * N, :].astype(F32)
                base = got_ref[at, 2 * N : 4 * N, :].astype(F32)
                new = base - step_size * (graft * precond)
                for w in range(2):
                    rows_f[slot, w, i * N : (i + 1) * N, :] = new[w * N : (w + 1) * N, :]
        for p in range(N):
            for w in range(2):
                cols = slice(j * HALF + w * LANES, j * HALF + (w + 1) * LANES)
                half_ref[p, :, cols] = rows_f[slot, w, pl.ds(p, N, stride=N), :].astype(BF16)
    graft_ref[...] = jnp.broadcast_to(graft, (N, LANES))


def join_kernel(got_ref, out_ref):
    for p in range(N):
        for j in range(N):
            for h in range(2):
                cols = slice(j * BLOCK + h * HALF, j * BLOCK + (h + 1) * HALF)
                out_ref[p, :, cols] = got_ref[h, p, :, j * HALF : (j + 1) * HALF]


def vmem(count):
    return [pl.BlockSpec(memory_space=pltpu.VMEM)] * count


def scratch(*shape, dtype):
    return pltpu.VMEM(shape, dtype)


def call(kernel, outs, scratches, flops=0, scalars=0, arrays=1, mib=32, space=pltpu.VMEM):
    return pl.pallas_call(
        kernel,
        out_shape=tuple(jax.ShapeDtypeStruct(*o) for o in outs),
        in_specs=[pl.BlockSpec(memory_space=pltpu.SMEM)] * scalars
        + [pl.BlockSpec(memory_space=space)] * arrays,
        out_specs=tuple(vmem(len(outs))),
        scratch_shapes=scratches,
        compiler_params=pltpu.CompilerParams(vmem_limit_bytes=mib * 1024 * 1024),
        cost_estimate=pl.CostEstimate(flops=flops, bytes_accessed=1 << 20, transcendentals=0),
    )


def step(gradients, left_stat, right_stat, momentum, master):
    own = (lax.axis_index("x") * 2 + lax.axis_index("co")).astype(jnp.int32).reshape(1)
    pieces, share = call(
        pack_kernel,
        [((N, 2 * ROWS, HALF), BF16), ((SHARE, BLOCK), BF16)],
        [
            scratch(N, N, N * BLOCK, dtype=BF16),
            scratch(4, ROWS, LANES, dtype=F32),
            scratch(4, ROWS, BLOCK, dtype=F32),
            pltpu.SemaphoreType.DMA((N,)),
            pltpu.SemaphoreType.DMA((4,)),
        ],
        arrays=5,
        mib=60,
        space=pltpu.HBM,
    )(gradients[0], left_stat[0], right_stat[0], momentum[0], master[0])
    s0 = turned(share)
    shares = [s0] + [along_x(s0, flip) for flip in (1, 2, 3)]
    twin = other_core(jnp.concatenate(shares, axis=0))

    pieces = exchanged(pieces, REP)
    mean = jnp.sum(pieces.astype(F32), axis=0) * (1.0 / N)
    mean = exchanged(mean.reshape(2 * N, N, HALF), PLANE)
    mean = spread(mean.reshape(2 * ROWS, HALF), "x")
    mean = spread(mean.reshape(BLOCK, HALF), "co")

    mean, grams, ret = call(
        gram_kernel,
        [((BLOCK, BLOCK), F32), ((2, BLOCK, BLOCK), F32), ((2 * ROWS, BLOCK), BF16)],
        [scratch(BLOCK, BLOCK, dtype=BF16)],
        flops=4 * BLOCK**3,
        scalars=1,
        mib=16,
    )(own, mean)
    ret = turned(ret)
    update = call(
        block_kernel,
        [((8 * N, MESSAGE, LANES), BF16), ((ROWS, BLOCK), BF16)],
        [
            scratch(2, BLOCK, BLOCK, dtype=F32),
            scratch(2, BLOCK, BLOCK, dtype=BF16),
            scratch(2, BLOCK, BLOCK, dtype=BF16),
            scratch(2, BLOCK, BLOCK, dtype=F32),
            scratch(2, BLOCK, BLOCK, dtype=BF16),
            scratch(BLOCK, BLOCK, dtype=F32),
            scratch(BLOCK, BLOCK, dtype=BF16),
            scratch(BLOCK, BLOCK, dtype=BF16),
            scratch(BLOCK, BLOCK, dtype=F32),
        ],
        flops=52 * BLOCK**3,
        scalars=1,
        arrays=7,
    )
    messages, rows = update(own, mean, grams, *shares, twin)
    rows = turned(rows)
    messages, ret = lax.optimization_barrier((messages, ret))
    got = exchanged(messages, SOLID)
    ret, got = lax.optimization_barrier((ret, got))
    half, graft = call(
        weight_kernel,
        [((N, N, N * HALF), BF16), ((N, LANES), F32)],
        [scratch(2, 2, ROWS, LANES, dtype=F32)],
        mib=16,
    )(got)
    half = spread(half, "co")
    (params,) = call(join_kernel, [((N, N, N * BLOCK), BF16)], [], mib=8)(half)
    moment_rows = moment_decay * momentum[0] + graft[0, 0] * rows.astype(F32)
    left_next = stat_decay * left_stat[0] + (1.0 - stat_decay) * ret[:ROWS].astype(F32)
    right_next = stat_decay * right_stat[0] + (1.0 - stat_decay) * ret[ROWS:].astype(F32)
    return (params, moment_rows[None], left_next[None], right_next[None])


def solution(mesh):
    split = Mesh(mesh.devices.reshape(SIZES), ALL)
    in_specs = (P(REP, BLK, None, None),) + (P(BLK, REP, None),) * 4
    out_specs = (P(BLK, None, None),) + (P(BLK, REP, None),) * 3
    return jax.shard_map(step, mesh=split, in_specs=in_specs, out_specs=out_specs, check_vma=False)
```

```python
import jax
import jax.numpy as jnp
from jax import lax
from jax.experimental import pallas as pl
from jax.experimental.pallas import tpu as pltpu
from jax.sharding import Mesh
from jax.sharding import PartitionSpec as P

REP = ("zl", "co")
ALL = ("zl", "co", "zh", "x", "y")
BLK = ("zh", "x", "y")
PLANE = ("zh", "y")
SOLID = ("zl", "zh", "y")
SIZES = (4, 2, 2, 4, 8)
N = 8
ROWS = 64
BLOCK = 512
ITERS = 4
LANES = 128
HALF = BLOCK // 2
SHARE = 3 * ROWS
MESSAGE = 40
WIDE = BLOCK // LANES

stat_decay = 0.9
moment_decay = 0.9
step_size = 0.25

F32 = jnp.float32
BF16 = jnp.bfloat16


def exchanged(pieces, axis):
    return lax.all_to_all(pieces, axis, split_axis=0, concat_axis=0, tiled=True)


def moved(shard, move):
    sizes = SIZES

    def place(where):
        index = 0
        for size, value in zip(sizes, where):
            index = index * size + value
        return index

    def device(index):
        where = []
        for size in reversed(sizes):
            where.append(index % size)
            index //= size
        return tuple(reversed(where))

    count = 1
    for size in sizes:
        count *= size
    pairs = [(k, place(move(*device(k)))) for k in range(count)]
    return lax.ppermute(shard, ALL, pairs)


def turned(shard):
    return moved(shard, lambda zl, co, zh, x, y: (x, co, zh, zl, y))


def along_x(shard, flip):
    return moved(shard, lambda zl, co, zh, x, y: (zl, co, zh, x ^ flip, y))


def other_core(shard):
    return moved(shard, lambda zl, co, zh, x, y: (zl, 1 - co, zh, x, y))


def spread(shard, axis):
    copies = jnp.broadcast_to(shard[None], (lax.axis_size(axis), *shard.shape))
    return exchanged(copies, axis)


def three_parts(value):
    high = value.astype(BF16).astype(F32)
    rest = value - high
    middle = rest.astype(BF16).astype(F32)
    return high, middle, rest - middle


def dot(a, b, dims=((1,), (0,))):
    return lax.dot_general(a, b, (dims, ((), ())), preferred_element_type=F32)


def pack_kernel(grad_ref, out_ref, rows_f):
    for j in range(N):
        for w in range(WIDE):
            slot = (j * WIDE + w) % 4
            for p in range(N):
                cols = slice(j * BLOCK + w * LANES, j * BLOCK + (w + 1) * LANES)
                rows_f[slot, p * N : (p + 1) * N, :] = grad_ref[p, :, cols].astype(F32)
            lanes = slice(w % 2 * LANES, (w % 2 + 1) * LANES)
            for i in range(N):
                at = (i // 4 * N + j) * N
                rows = rows_f[slot, pl.ds(i, N, stride=N), :]
                out_ref[i % 4 * 2 + w // 2, at : at + N, lanes] = rows.astype(BF16)


def block_kernel(
    own_ref, got_ref, s0_ref, s1_ref, s2_ref, s3_ref, twin_ref,
    msg_ref, ret_ref, m_f, m_b, v_b, w_f, w_b, y_f, y_b, z_b, base_f,
):
    own = pl.multiple_of(own_ref[0] * ROWS, ROWS)
    x = own_ref[0] >> 1
    co = own_ref[0] & 1
    chunk = BLOCK // 2
    spans = [pl.ds(k * chunk, chunk) for k in range(2)]
    norm_g = jnp.zeros((1, 1), F32)
    for half in range(2):
        cols = slice(half * HALF, (half + 1) * HALF)
        for k in range(4):
            for zh in range(2):
                at = (k * 2 + zh) * ROWS
                part = got_ref[half, at : at + ROWS, :]
                norm_g += jnp.sum(part * part, keepdims=True)
                rows = slice((zh * 4 + k) * ROWS, (zh * 4 + k + 1) * ROWS)
                y_f[rows, cols] = part
                y_b[rows, cols] = part.astype(BF16)
    shares = []
    for flip, ref in enumerate((s0_ref, s1_ref, s2_ref, s3_ref)):
        shares.append((pl.multiple_of((own_ref[0] ^ (2 * flip)) * ROWS, ROWS), ref, 0))
        shares.append((pl.multiple_of((own_ref[0] ^ (2 * flip + 1)) * ROWS, ROWS), twin_ref, flip * SHARE))
    scale = jnp.ones((1, 1), F32)
    for side in range(2):
        w_f[side] = dot(y_b[...], y_b[...], (((1,), (1,)), ((0,), (0,)))[side])
        rows = w_f[side, pl.ds(own, ROWS), :]
        ret_ref[(1 + side) * ROWS : (2 + side) * ROWS, :] = rows.astype(BF16)
        total = jnp.zeros((1, 1), F32)
        for at, ref, start in shares:
            rows = pl.ds(at, ROWS)
            old = ref[start + side * ROWS : start + (side + 1) * ROWS, :].astype(F32)
            new = stat_decay * old + (1.0 - stat_decay) * w_f[side, rows, :]
            m_f[side, rows, :] = new
            total += jnp.sum(new * new, keepdims=True)
        frob = jnp.sqrt(total)
        scale = scale / jnp.sqrt(jnp.sqrt(frob))
        inverse = 1.0 / frob
        for rows in spans:
            new = m_f[side, rows, :] * inverse
            m_f[side, rows, :] = new
            m_b[side, rows, :] = new.astype(BF16)
    for at, ref, start in shares:
        base_f[pl.ds(at, ROWS), :] = ref[start + 2 * ROWS : start + 3 * ROWS, :].astype(F32)

    def apply_factors():
        for rows in spans:
            new = 1.25 * y_f[rows, :] - 0.25 * dot(m_b[0, rows, :], y_b[...])
            y_f[rows, :] = new
            z_b[rows, :] = new.astype(BF16)
        for rows in spans:
            new = 1.25 * y_f[rows, :] - 0.25 * dot(z_b[rows, :], m_b[1])
            y_f[rows, :] = new
            y_b[rows, :] = new.astype(BF16)

    def sweep(_, carry):
        for side in range(2):
            for rows in spans:
                square = dot(m_b[side, rows, :], m_b[side])
                v_b[side, rows, :] = (0.0625 * square - 0.625 * m_f[side, rows, :]).astype(BF16)
        apply_factors()
        for side in range(2):
            for rows in spans:
                new = 1.5625 * m_f[side, rows, :] + dot(v_b[side, rows, :], m_b[side])
                w_f[side, rows, :] = new
                w_b[side, rows, :] = new.astype(BF16)
        for side in range(2):
            for rows in spans:
                new = 1.5625 * w_f[side, rows, :] + dot(v_b[side, rows, :], w_b[side])
                m_f[side, rows, :] = new
                m_b[side, rows, :] = new.astype(BF16)
        return carry

    lax.fori_loop(0, ITERS - 1, sweep, 0)
    apply_factors()
    norm_p = jnp.zeros((1, 1), F32)
    for rows in spans:
        new = y_f[rows, :] * scale
        norm_p += jnp.sum(new * new, keepdims=True)
        y_f[rows, :] = new
    ret_ref[0:ROWS, :] = y_f[pl.ds(own, ROWS), :].astype(BF16)
    lane = lax.broadcasted_iota(jnp.int32, (N, LANES), 1)
    norms = jnp.zeros((N, LANES), F32)
    for k, part in enumerate(three_parts(norm_p) + three_parts(norm_g)):
        norms = jnp.where(lane == k, part, norms)
    norms = norms.astype(BF16)
    for zh in range(2):
        for row in range(N):
            rows = pl.ds(pl.multiple_of((zh * 4 + x) * ROWS + row * N, N), N)
            for k, ref in enumerate((y_f, base_f)):
                whole = ref[rows, :]
                half = jnp.where(co == 0, whole[:, :HALF], whole[:, HALF:])
                both = jnp.concatenate([half[:, :LANES], half[:, LANES:]], axis=0)
                both = both.astype(BF16)
                for z in range(4):
                    at = (z * 2 + zh) * N + row
                    msg_ref[at, k * 2 * N : (k + 1) * 2 * N, :] = both
            for z in range(4):
                msg_ref[(z * 2 + zh) * N + row, 4 * N : 5 * N, :] = norms


def weight_kernel(got_ref, half_ref, graft_ref, rows_f):
    total = jnp.zeros((N, LANES), F32)
    for k in range(8 * N):
        total += got_ref[k, 4 * N : 5 * N, :].astype(F32)
    lane = lax.broadcasted_iota(jnp.int32, (N, LANES), 1)
    norm_p = jnp.sum(jnp.where(lane < 3, total, 0.0), keepdims=True) * (1.0 / N)
    norm_g = jnp.sum(jnp.where(lane < 3, 0.0, total), keepdims=True) * (1.0 / N)
    graft = jnp.sqrt(norm_g) / jnp.sqrt(norm_p)
    for j in range(N):
        slot = j % 2
        for zh in range(2):
            for z in range(4):
                i = zh * 4 + z
                at = (z * 2 + zh) * N + j
                precond = got_ref[at, 0 : 2 * N, :].astype(F32)
                base = got_ref[at, 2 * N : 4 * N, :].astype(F32)
                new = base - step_size * (graft * precond)
                for w in range(2):
                    rows_f[slot, w, i * N : (i + 1) * N, :] = new[w * N : (w + 1) * N, :]
        for p in range(N):
            for w in range(2):
                cols = slice(j * HALF + w * LANES, j * HALF + (w + 1) * LANES)
                half_ref[p, :, cols] = rows_f[slot, w, pl.ds(p, N, stride=N), :].astype(BF16)
    graft_ref[...] = jnp.broadcast_to(graft, (N, LANES))


def join_kernel(got_ref, out_ref):
    for p in range(N):
        for j in range(N):
            for h in range(2):
                cols = slice(j * BLOCK + h * HALF, j * BLOCK + (h + 1) * HALF)
                out_ref[p, :, cols] = got_ref[h, p, :, j * HALF : (j + 1) * HALF]


def vmem(count):
    return [pl.BlockSpec(memory_space=pltpu.VMEM)] * count


def scratch(*shape, dtype):
    return pltpu.VMEM(shape, dtype)


def call(kernel, outs, scratches, flops=0, scalars=0, arrays=1, mib=32):
    return pl.pallas_call(
        kernel,
        out_shape=tuple(jax.ShapeDtypeStruct(*o) for o in outs),
        in_specs=[pl.BlockSpec(memory_space=pltpu.SMEM)] * scalars + vmem(arrays),
        out_specs=tuple(vmem(len(outs))),
        scratch_shapes=scratches,
        compiler_params=pltpu.CompilerParams(vmem_limit_bytes=mib * 1024 * 1024),
        cost_estimate=pl.CostEstimate(flops=flops, bytes_accessed=1 << 20, transcendentals=0),
    )


def step(gradients, left_stat, right_stat, momentum, master):
    own = (lax.axis_index("x") * 2 + lax.axis_index("co")).astype(jnp.int32).reshape(1)
    base = master[0] - (step_size * moment_decay) * momentum[0]
    share = jnp.concatenate([a.astype(BF16) for a in (left_stat[0], right_stat[0], base)], axis=0)
    s0 = turned(share)
    shares = [s0] + [along_x(s0, flip) for flip in (1, 2, 3)]
    twin = other_core(jnp.concatenate(shares, axis=0))
    (pieces,) = call(
        pack_kernel, [((N, 2 * ROWS, HALF), BF16)], [scratch(4, ROWS, LANES, dtype=F32)], mib=8
    )(gradients[0])
    pieces = exchanged(pieces, REP)
    mean = jnp.sum(pieces.astype(F32), axis=0) * (1.0 / N)
    mean = exchanged(mean.reshape(2 * N, N, HALF), PLANE)
    mean = spread(mean.reshape(2 * ROWS, HALF), "x")
    mean = spread(mean.reshape(BLOCK, HALF), "co")
    update = call(
        block_kernel,
        [((8 * N, MESSAGE, LANES), BF16), ((SHARE, BLOCK), BF16)],
        [
            scratch(2, BLOCK, BLOCK, dtype=F32),
            scratch(2, BLOCK, BLOCK, dtype=BF16),
            scratch(2, BLOCK, BLOCK, dtype=BF16),
            scratch(2, BLOCK, BLOCK, dtype=F32),
            scratch(2, BLOCK, BLOCK, dtype=BF16),
            scratch(BLOCK, BLOCK, dtype=F32),
            scratch(BLOCK, BLOCK, dtype=BF16),
            scratch(BLOCK, BLOCK, dtype=BF16),
            scratch(BLOCK, BLOCK, dtype=F32),
        ],
        flops=56 * BLOCK**3,
        scalars=1,
        arrays=6,
    )
    messages, ret = update(own, mean, *shares, twin)
    ret = turned(ret)
    got = exchanged(messages, SOLID)
    half, graft = call(
        weight_kernel,
        [((N, N, N * HALF), BF16), ((N, LANES), F32)],
        [scratch(2, 2, ROWS, LANES, dtype=F32)],
        mib=16,
    )(got)
    half = spread(half, "co")
    (params,) = call(join_kernel, [((N, N, N * BLOCK), BF16)], [], mib=8)(half)
    ret, graft = lax.optimization_barrier((ret, graft))
    moment_rows = moment_decay * momentum[0] + graft[0, 0] * ret[:ROWS].astype(F32)
    left_next = stat_decay * left_stat[0] + (1.0 - stat_decay) * ret[ROWS : 2 * ROWS].astype(F32)
    right_next = stat_decay * right_stat[0] + (1.0 - stat_decay) * ret[2 * ROWS :].astype(F32)
    return (params, moment_rows[None], left_next[None], right_next[None])


def solution(mesh):
    split = Mesh(mesh.devices.reshape(SIZES), ALL)
    in_specs = (P(REP, BLK, None, None),) + (P(BLK, REP, None),) * 4
    out_specs = (P(BLK, None, None),) + (P(BLK, REP, None),) * 3
    return jax.shard_map(step, mesh=split, in_specs=in_specs, out_specs=out_specs, check_vma=False)
```

```python
import jax
import jax.numpy as jnp
from jax import lax
from jax.experimental import pallas as pl
from jax.experimental.pallas import tpu as pltpu
from jax.sharding import Mesh
from jax.sharding import PartitionSpec as P

REP = ("zl", "co")
ALL = ("zl", "co", "zh", "x", "y")
BLK = ("zh", "x", "y")
PLANE = ("zh", "y")
SOLID = ("zl", "zh", "y")
SIZES = (4, 2, 2, 4, 8)
N = 8
ROWS = 64
BLOCK = 512
ITERS = 4
LANES = 128
HALF = BLOCK // 2
SHARE = 3 * ROWS
MESSAGE = 40
DEEP = 4 * ROWS + 2 * SHARE
WIDE = BLOCK // LANES

stat_decay = 0.9
moment_decay = 0.9
step_size = 0.25

F32 = jnp.float32
BF16 = jnp.bfloat16


def exchanged(pieces, axis):
    return lax.all_to_all(pieces, axis, split_axis=0, concat_axis=0, tiled=True)


def moved(shard, move):
    sizes = SIZES

    def place(where):
        index = 0
        for size, value in zip(sizes, where):
            index = index * size + value
        return index

    def device(index):
        where = []
        for size in reversed(sizes):
            where.append(index % size)
            index //= size
        return tuple(reversed(where))

    count = 1
    for size in sizes:
        count *= size
    pairs = [(k, place(move(*device(k)))) for k in range(count)]
    return lax.ppermute(shard, ALL, pairs)


def turned(shard):
    return moved(shard, lambda zl, co, zh, x, y: (x, co, zh, zl, y))


def spread(shard, axis):
    copies = jnp.broadcast_to(shard[None], (lax.axis_size(axis), *shard.shape))
    return exchanged(copies, axis)


def three_parts(value):
    high = value.astype(BF16).astype(F32)
    rest = value - high
    middle = rest.astype(BF16).astype(F32)
    return high, middle, rest - middle


def dot(a, b, dims=((1,), (0,))):
    return lax.dot_general(a, b, (dims, ((), ())), preferred_element_type=F32)


def pack_kernel(grad_ref, out_ref, rows_f):
    for j in range(N):
        for w in range(WIDE):
            slot = (j * WIDE + w) % 4
            for p in range(N):
                cols = slice(j * BLOCK + w * LANES, j * BLOCK + (w + 1) * LANES)
                rows_f[slot, p * N : (p + 1) * N, :] = grad_ref[p, :, cols].astype(F32)
            lanes = slice(w % 2 * LANES, (w % 2 + 1) * LANES)
            for i in range(N):
                at = (i // 4 * N + j) * N
                rows = rows_f[slot, pl.ds(i, N, stride=N), :]
                out_ref[i % 4 * 2 + w // 2, at : at + N, lanes] = rows.astype(BF16)


def ring_kernel(mean_ref, share_ref, out_ref):
    mean = mean_ref[...]
    high = mean.astype(BF16)
    low = (mean - high.astype(F32)).astype(BF16)
    for k in range(SIZES[3]):
        out_ref[k, 0 : 2 * ROWS, :] = high
        out_ref[k, 2 * ROWS : 4 * ROWS, :] = low
        for half in range(2):
            rows = slice(4 * ROWS + half * SHARE, 4 * ROWS + (half + 1) * SHARE)
            out_ref[k, rows, :] = share_ref[:, half * HALF : (half + 1) * HALF]


def block_kernel(
    own_ref, got_ref, msg_ref, ret_ref, m_f, m_b, v_b, w_f, w_b, y_f, y_b, z_b, base_f,
):
    own = pl.multiple_of(own_ref[0] * ROWS, ROWS)
    x = own_ref[0] >> 1
    co = own_ref[0] & 1
    chunk = BLOCK // 2
    spans = [pl.ds(k * chunk, chunk) for k in range(2)]
    norm_g = jnp.zeros((1, 1), F32)
    for half in range(2):
        cols = slice(half * HALF, (half + 1) * HALF)
        for k in range(4):
            for zh in range(2):
                at = zh * ROWS
                high = got_ref[half, k, at : at + ROWS, :]
                low = got_ref[half, k, 2 * ROWS + at : 3 * ROWS + at, :]
                part = high.astype(F32) + low.astype(F32)
                norm_g += jnp.sum(part * part, keepdims=True)
                rows = slice((zh * 4 + k) * ROWS, (zh * 4 + k + 1) * ROWS)
                y_f[rows, cols] = part
                y_b[rows, cols] = part.astype(BF16)
    scale = jnp.ones((1, 1), F32)
    for side in range(2):
        w_f[side] = dot(y_b[...], y_b[...], (((1,), (1,)), ((0,), (0,)))[side])
        rows = w_f[side, pl.ds(own, ROWS), :]
        ret_ref[(1 + side) * ROWS : (2 + side) * ROWS, :] = rows.astype(BF16)
        total = jnp.zeros((1, 1), F32)
        for k in range(N):
            rows = slice(k * ROWS, (k + 1) * ROWS)
            for half in range(2):
                cols = slice(half * HALF, (half + 1) * HALF)
                at = 4 * ROWS + half * SHARE + side * ROWS
                old = got_ref[k % 2, k // 2, at : at + ROWS, :].astype(F32)
                new = stat_decay * old + (1.0 - stat_decay) * w_f[side, rows, cols]
                m_f[side, rows, cols] = new
                total += jnp.sum(new * new, keepdims=True)
        frob = jnp.sqrt(total)
        scale = scale / jnp.sqrt(jnp.sqrt(frob))
        inverse = 1.0 / frob
        for rows in spans:
            new = m_f[side, rows, :] * inverse
            m_f[side, rows, :] = new
            m_b[side, rows, :] = new.astype(BF16)
    for k in range(N):
        for half in range(2):
            at = 4 * ROWS + half * SHARE + 2 * ROWS
            cols = slice(half * HALF, (half + 1) * HALF)
            base_f[k * ROWS : (k + 1) * ROWS, cols] = got_ref[k % 2, k // 2, at : at + ROWS, :].astype(F32)

    def apply_factors():
        for rows in spans:
            new = 1.25 * y_f[rows, :] - 0.25 * dot(m_b[0, rows, :], y_b[...])
            y_f[rows, :] = new
            z_b[rows, :] = new.astype(BF16)
        for rows in spans:
            new = 1.25 * y_f[rows, :] - 0.25 * dot(z_b[rows, :], m_b[1])
            y_f[rows, :] = new
            y_b[rows, :] = new.astype(BF16)

    def sweep(_, carry):
        for side in range(2):
            for rows in spans:
                square = dot(m_b[side, rows, :], m_b[side])
                v_b[side, rows, :] = (0.0625 * square - 0.625 * m_f[side, rows, :]).astype(BF16)
        apply_factors()
        for side in range(2):
            for rows in spans:
                new = 1.5625 * m_f[side, rows, :] + dot(v_b[side, rows, :], m_b[side])
                w_f[side, rows, :] = new
                w_b[side, rows, :] = new.astype(BF16)
        for side in range(2):
            for rows in spans:
                new = 1.5625 * w_f[side, rows, :] + dot(v_b[side, rows, :], w_b[side])
                m_f[side, rows, :] = new
                m_b[side, rows, :] = new.astype(BF16)
        return carry

    lax.fori_loop(0, ITERS - 1, sweep, 0)
    apply_factors()
    norm_p = jnp.zeros((1, 1), F32)
    for rows in spans:
        new = y_f[rows, :] * scale
        norm_p += jnp.sum(new * new, keepdims=True)
        y_f[rows, :] = new
    ret_ref[0:ROWS, :] = y_f[pl.ds(own, ROWS), :].astype(BF16)
    lane = lax.broadcasted_iota(jnp.int32, (N, LANES), 1)
    norms = jnp.zeros((N, LANES), F32)
    for k, part in enumerate(three_parts(norm_p) + three_parts(norm_g)):
        norms = jnp.where(lane == k, part, norms)
    norms = norms.astype(BF16)
    for zh in range(2):
        for row in range(N):
            rows = pl.ds(pl.multiple_of((zh * 4 + x) * ROWS + row * N, N), N)
            for k, ref in enumerate((y_f, base_f)):
                whole = ref[rows, :]
                half = jnp.where(co == 0, whole[:, :HALF], whole[:, HALF:])
                both = jnp.concatenate([half[:, :LANES], half[:, LANES:]], axis=0)
                both = both.astype(BF16)
                for z in range(4):
                    at = (z * 2 + zh) * N + row
                    msg_ref[at, k * 2 * N : (k + 1) * 2 * N, :] = both
            for z in range(4):
                msg_ref[(z * 2 + zh) * N + row, 4 * N : 5 * N, :] = norms


def weight_kernel(got_ref, half_ref, graft_ref, rows_f):
    total = jnp.zeros((N, LANES), F32)
    for k in range(8 * N):
        total += got_ref[k, 4 * N : 5 * N, :].astype(F32)
    lane = lax.broadcasted_iota(jnp.int32, (N, LANES), 1)
    norm_p = jnp.sum(jnp.where(lane < 3, total, 0.0), keepdims=True) * (1.0 / N)
    norm_g = jnp.sum(jnp.where(lane < 3, 0.0, total), keepdims=True) * (1.0 / N)
    graft = jnp.sqrt(norm_g) / jnp.sqrt(norm_p)
    for j in range(N):
        slot = j % 2
        for zh in range(2):
            for z in range(4):
                i = zh * 4 + z
                at = (z * 2 + zh) * N + j
                precond = got_ref[at, 0 : 2 * N, :].astype(F32)
                base = got_ref[at, 2 * N : 4 * N, :].astype(F32)
                new = base - step_size * (graft * precond)
                for w in range(2):
                    rows_f[slot, w, i * N : (i + 1) * N, :] = new[w * N : (w + 1) * N, :]
        for p in range(N):
            for w in range(2):
                cols = slice(j * HALF + w * LANES, j * HALF + (w + 1) * LANES)
                half_ref[p, :, cols] = rows_f[slot, w, pl.ds(p, N, stride=N), :].astype(BF16)
    graft_ref[...] = jnp.broadcast_to(graft, (N, LANES))


def join_kernel(got_ref, out_ref):
    for p in range(N):
        for j in range(N):
            for h in range(2):
                cols = slice(j * BLOCK + h * HALF, j * BLOCK + (h + 1) * HALF)
                out_ref[p, :, cols] = got_ref[h, p, :, j * HALF : (j + 1) * HALF]


def vmem(count):
    return [pl.BlockSpec(memory_space=pltpu.VMEM)] * count


def scratch(*shape, dtype):
    return pltpu.VMEM(shape, dtype)


def call(kernel, outs, scratches, flops=0, scalars=0, arrays=1, mib=32):
    return pl.pallas_call(
        kernel,
        out_shape=tuple(jax.ShapeDtypeStruct(*o) for o in outs),
        in_specs=[pl.BlockSpec(memory_space=pltpu.SMEM)] * scalars + vmem(arrays),
        out_specs=tuple(vmem(len(outs))),
        scratch_shapes=scratches,
        compiler_params=pltpu.CompilerParams(vmem_limit_bytes=mib * 1024 * 1024),
        cost_estimate=pl.CostEstimate(flops=flops, bytes_accessed=1 << 20, transcendentals=0),
    )


def step(gradients, left_stat, right_stat, momentum, master):
    own = (lax.axis_index("x") * 2 + lax.axis_index("co")).astype(jnp.int32).reshape(1)
    base = master[0] - (step_size * moment_decay) * momentum[0]
    share = jnp.concatenate([a.astype(BF16) for a in (left_stat[0], right_stat[0], base)], axis=0)
    s0 = turned(share)
    (pieces,) = call(
        pack_kernel, [((N, 2 * ROWS, HALF), BF16)], [scratch(4, ROWS, LANES, dtype=F32)], mib=8
    )(gradients[0])
    pieces = exchanged(pieces, REP)
    mean = jnp.sum(pieces.astype(F32), axis=0) * (1.0 / N)
    mean = exchanged(mean.reshape(2 * N, N, HALF), PLANE)
    (message,) = call(ring_kernel, [((SIZES[3], DEEP, HALF), BF16)], [], arrays=2, mib=8)(
        mean.reshape(2 * ROWS, HALF), s0
    )
    message = exchanged(message, "x")
    both = spread(message, "co")
    update = call(
        block_kernel,
        [((8 * N, MESSAGE, LANES), BF16), ((SHARE, BLOCK), BF16)],
        [
            scratch(2, BLOCK, BLOCK, dtype=F32),
            scratch(2, BLOCK, BLOCK, dtype=BF16),
            scratch(2, BLOCK, BLOCK, dtype=BF16),
            scratch(2, BLOCK, BLOCK, dtype=F32),
            scratch(2, BLOCK, BLOCK, dtype=BF16),
            scratch(BLOCK, BLOCK, dtype=F32),
            scratch(BLOCK, BLOCK, dtype=BF16),
            scratch(BLOCK, BLOCK, dtype=BF16),
            scratch(BLOCK, BLOCK, dtype=F32),
        ],
        flops=56 * BLOCK**3,
        scalars=1,
    )
    messages, ret = update(own, both)
    got = exchanged(messages, SOLID)
    ret, got = lax.optimization_barrier((ret, got))
    ret = turned(ret)
    half, graft = call(
        weight_kernel,
        [((N, N, N * HALF), BF16), ((N, LANES), F32)],
        [scratch(2, 2, ROWS, LANES, dtype=F32)],
        mib=16,
    )(got)
    half = spread(half, "co")
    (params,) = call(join_kernel, [((N, N, N * BLOCK), BF16)], [], mib=8)(half)
    ret, graft = lax.optimization_barrier((ret, graft))
    moment_rows = moment_decay * momentum[0] + graft[0, 0] * ret[:ROWS].astype(F32)
    left_next = stat_decay * left_stat[0] + (1.0 - stat_decay) * ret[ROWS : 2 * ROWS].astype(F32)
    right_next = stat_decay * right_stat[0] + (1.0 - stat_decay) * ret[2 * ROWS :].astype(F32)
    return (params, moment_rows[None], left_next[None], right_next[None])


def solution(mesh):
    split = Mesh(mesh.devices.reshape(SIZES), ALL)
    in_specs = (P(REP, BLK, None, None),) + (P(BLK, REP, None),) * 4
    out_specs = (P(BLK, None, None),) + (P(BLK, REP, None),) * 3
    return jax.shard_map(step, mesh=split, in_specs=in_specs, out_specs=out_specs, check_vma=False)
```
